1024 devices in a mesh: heads: 16 (over y, core), seq: 64 (over x, z).
Axes of the slice: x: 4, y: 8, z: 16, core: 2. Of those that a mesh axis runs over, the one named last changes fastest.
Arguments:
- queries: bfloat16 [8192, 64, 576], P('seq', 'heads'), may hold values from -6 to 6
- latents: bfloat16 [64, 128, 576], P('seq', 'heads'), may hold values from -6 to 6
- grad_out: bfloat16 [8192, 64, 512], P('seq', 'heads'), may hold values from -6 to 6
- selected: int32 [64, 4], P('seq'), may hold values from 0 to 63, as said below
Outputs:
- output: bfloat16 [8192, 64, 512], P('seq', 'heads')
- grad_query: bfloat16 [8192, 64, 576], P('seq', 'heads')
- latent_grad: float32 [64, 128, 576], P('seq', 'heads')
The draws below stay inside these ranges and needn't reach their ends.
Inputs may be any that keep to these rules, and one draw needn't show every extreme that they name: `selected`: row i lists 4 different blocks, none of them held on the same index of seq as block i (blocks i and j share it when i // 1 equals j // 1); how often a block is chosen varies widely between blocks.
All inputs are finite; a program needn't handle non-finite values.
Results may differ from the reference program's by a relative error of at most 0.012.
Values may be sent and summed in bfloat16 or wider, within the bound.
No kernel may reach another device: no remote copies, remote signals or barrier semaphores. Data moves between devices by JAX's collectives and lax.ppermute only.
A program may use at most 32 MiB of HBM per device.

```python
import jax
import jax.numpy as jnp
from jax import lax

HEADS = 64
LATENT = 512
BLOCK = 128
TOP = 4
DK = 576
QUERY_BLOCK_UNIT = 1
SEQ = 8192
NBLK = 64


def draw_latents(key, part):
    values = jnp.clip(jax.random.normal(jax.random.fold_in(key, 11), (NBLK, BLOCK, DK), jnp.float32), -6.0, 6.0)
    return values.astype(jnp.bfloat16)


def draw_queries(key, part):
    values = jnp.clip(jax.random.normal(jax.random.fold_in(key, 12), (SEQ, HEADS, DK), jnp.float32), -6.0, 6.0)
    return values.astype(jnp.bfloat16)


def draw_selected(key, part):
    popular = jax.random.randint(jax.random.fold_in(key, 21), (NBLK,), 0, 5)
    weight = (popular + 1) * (popular + 1)
    noise = jax.random.randint(jax.random.fold_in(key, 22), (NBLK, NBLK), 0, 4096)
    column_span = jnp.arange(NBLK, dtype=jnp.int32)
    scores = noise * weight[None, :] * NBLK + column_span[None, :]
    holder = column_span // QUERY_BLOCK_UNIT
    scores = jnp.where(holder[:, None] == holder[None, :], -1, scores)
    _, chosen = lax.top_k(scores, TOP)
    return chosen.astype(jnp.int32)


def levels(key, shape, split, smallest, top_value):
    loudness, own = 1.0, jax.random.fold_in(key, 6)
    for axis_at, shards_of in split:
        steps = jnp.exp(jax.random.uniform(jax.random.fold_in(own, axis_at), (shards_of,), jnp.float32, smallest / len(split), top_value / len(split)))
        loudness = loudness * jnp.repeat(steps, shape[axis_at] // shards_of).reshape([-1 if axis == axis_at else 1 for axis in range(len(shape))])
    return loudness


def scatter_about(key, shape, spread, bound, shards=(), kind=jnp.bfloat16):
    array = spread * jax.random.normal(key, shape, jnp.float32)
    if shards:
        array = array * levels(key, shape, shards, -0.22, 0.18)
    return jnp.clip(array, -bound, bound).astype(kind)


def setup_inputs(seed: int = 0) -> dict:
    arg_keys = jax.random.split(jax.random.key(seed), 5)
    return {
        "queries": draw_queries(jax.random.fold_in(arg_keys[4], 71), 0),
        "latents": draw_latents(jax.random.fold_in(arg_keys[4], 71), 0),
        "grad_out": scatter_about(arg_keys[2], (SEQ, HEADS, LATENT), 1.0, 6.0, ((0, 64), (1, 16))),
        "selected": draw_selected(jax.random.fold_in(arg_keys[4], 71), 0),
    }


def reference(queries, latents, grad_out, selected):
    list_blocks, block_size, key_width = latents.shape
    token_total, head_count, _ = queries.shape
    value_width = grad_out.shape[2]
    score_scale = key_width ** -0.5
    query_blocks = queries.reshape(list_blocks, block_size, head_count, key_width)
    grad_blocks = grad_out.reshape(list_blocks, block_size, head_count, value_width)
    own_blocks = jnp.arange(list_blocks, dtype=jnp.int32)[:, None]
    block_ids = jnp.concatenate([own_blocks, selected.astype(jnp.int32)], axis=1)

    def block_step(totals, pieces):
        query_row_tiles, grad_rows, key_ids = pieces
        key_row_tiles = latents[key_ids].reshape(-1, key_width).astype(jnp.float32)
        query_full = query_row_tiles.astype(jnp.float32)
        grad_full = grad_rows.astype(jnp.float32)
        value_rows = key_row_tiles[:, :value_width]
        scores = jnp.einsum('thd,kd->htk', query_full, key_row_tiles) * score_scale
        prob_full = jax.nn.softmax(scores, axis=-1)
        prob_half = prob_full.astype(jnp.bfloat16)
        output = jnp.einsum('htk,kl->thl', prob_half.astype(jnp.float32), value_rows).astype(jnp.bfloat16)
        row_delta = jnp.sum(grad_full * output.astype(jnp.float32), axis=-1)
        grad_prob = jnp.einsum('thl,kl->htk', grad_full, value_rows)
        score_gradient = (prob_full * (grad_prob - row_delta.T[:, :, None]) * score_scale).astype(jnp.bfloat16)
        grad_query = jnp.einsum('htk,kd->thd', score_gradient.astype(jnp.float32), key_row_tiles).astype(jnp.bfloat16)
        key_gradient = jnp.einsum('htk,thd->kd', score_gradient.astype(jnp.float32), query_full)
        grad_value = jnp.einsum('htk,thl->kl', prob_half.astype(jnp.float32), grad_full)
        key_gradient = key_gradient.at[:, :value_width].add(grad_value)
        totals = totals.at[key_ids].add(key_gradient.reshape(-1, block_size, key_width))
        return totals, (output, grad_query)

    start_grad = jnp.zeros((list_blocks, block_size, key_width), jnp.float32)
    latent_grad, (output, grad_query) = lax.scan(block_step, start_grad, (query_blocks, grad_blocks, block_ids))
    return (output.reshape(token_total, head_count, value_width),
            grad_query.reshape(token_total, head_count, key_width),
            latent_grad)
```

```python
import jax
import jax.numpy as jnp
from jax import lax
from jax.sharding import Mesh
from jax.sharding import PartitionSpec as P

SEQ = ("sx", "sz")
HEADS = ("hy", "hc")


def swap(tiles, axis):
    return lax.all_to_all(tiles, axis, 0, 0, tiled=True)


def summed(tiles):
    return jnp.sum(tiles.astype(jnp.float32), axis=0)


def shards(queries, latents, grad_out, selected):
    row_share, key_width = latents.shape[1:]
    token_total, head_count, _ = queries.shape
    value_width = grad_out.shape[2]
    key_blocks = selected.shape[1] + 1
    cores = lax.axis_size("hc")
    chips = lax.axis_size("hy")
    block_size = row_share * cores * chips
    nx, nz = (lax.axis_size(a) for a in SEQ)
    list_blocks = nx * nz
    score_scale = key_width ** (-0.5)

    slices = lax.all_gather(latents, "sz", axis=0, tiled=True)
    slices = lax.all_gather(slices, "sx", axis=0, tiled=True)
    own = lax.axis_index(SEQ).astype(jnp.int32)
    block_ids = jnp.concatenate([own[None], selected[0]])
    picked = jnp.take(slices, block_ids, axis=0)
    keys = lax.all_gather(picked, HEADS, axis=1, tiled=True)
    keys = keys.reshape(key_blocks * block_size, key_width)
    values = keys[:, :value_width]

    scores = jnp.einsum("thd,kd->htk", queries, keys, preferred_element_type=jnp.float32) * score_scale
    probs = jax.nn.softmax(scores, axis=-1)
    half = probs.astype(jnp.bfloat16)
    output = jnp.einsum("htk,kl->thl", half, values, preferred_element_type=jnp.float32).astype(jnp.bfloat16)
    row_delta = jnp.sum(grad_out.astype(jnp.float32) * output.astype(jnp.float32), axis=-1)
    grad_prob = jnp.einsum("thl,kl->htk", grad_out, values, preferred_element_type=jnp.float32)
    grad_score = (probs * (grad_prob - row_delta.T[..., None]) * score_scale).astype(jnp.bfloat16)
    grad_query = jnp.einsum("htk,kd->thd", grad_score, keys, preferred_element_type=jnp.float32).astype(jnp.bfloat16)
    key_grad = jnp.einsum("htk,thd->kd", grad_score, queries, preferred_element_type=jnp.float32)
    value_grad = jnp.einsum("htk,thl->kl", half, grad_out, preferred_element_type=jnp.float32)
    contrib = jnp.concatenate([key_grad[:, :value_width] + value_grad, key_grad[:, value_width:]], axis=-1)

    bundles = contrib.astype(jnp.bfloat16).reshape(key_blocks, chips, cores, row_share, key_width)
    bundles = bundles.transpose(2, 1, 0, 3, 4)
    bundles = summed(swap(bundles, "hc")).astype(jnp.bfloat16)
    share = summed(swap(bundles, "hy")).astype(jnp.bfloat16)
    one_hot = (jnp.arange(list_blocks, dtype=jnp.int32)[:, None] == block_ids[None, :]).astype(jnp.bfloat16)
    dense = jnp.dot(one_hot, share.reshape(key_blocks, -1), preferred_element_type=jnp.float32)
    dense = dense.astype(jnp.bfloat16).reshape(nx, nz, row_share, key_width)
    dense = summed(swap(dense, "sx")).astype(jnp.bfloat16)
    latent_grad = summed(swap(dense, "sz"))
    return output, grad_query, latent_grad[None]


def solution(mesh):
    split = Mesh(mesh.devices.reshape(mesh.shape["heads"] // 2, 2, 4, 16), ("hy", "hc", "sx", "sz"))
    placed = P(SEQ, HEADS, None)
    return jax.shard_map(
        shards,
        mesh=split,
        in_specs=(placed, placed, placed, P(SEQ, None)),
        out_specs=(placed, placed, placed),
        check_vma=False,
    )
```

```python
import functools

import jax
import jax.numpy as jnp
from jax import lax
from jax.experimental import pallas as pl
from jax.experimental.pallas import tpu as pltpu
from jax.sharding import Mesh
from jax.sharding import PartitionSpec as P

SEQ = ("sx", "sz")
HEADS = ("hy", "hc")
F32 = jnp.float32
BF16 = jnp.bfloat16
VMEM = pl.BlockSpec(memory_space=pltpu.VMEM)
SMEM = pl.BlockSpec(memory_space=pltpu.SMEM)


def swap(tiles, axis):
    return lax.all_to_all(tiles, axis, 0, 0, tiled=True)


def dot(a, b, dims=((1,), (0,))):
    return lax.dot_general(a, b, (dims, ((), ())), preferred_element_type=F32)


def order_matrix(tokens, heads, transposed=False):
    size = tokens * heads
    rows = lax.broadcasted_iota(jnp.int32, (size, size), 1 if transposed else 0)
    cols = lax.broadcasted_iota(jnp.int32, (size, size), 0 if transposed else 1)
    return ((rows % tokens) * heads + rows // tokens == cols).astype(BF16)


def pick_kernel(own_ref, selected_ref, slices_ref, picked_ref):
    rows = slices_ref.shape[1]
    picked_ref[pl.ds(0, rows), :] = slices_ref[own_ref[0]]
    for k in range(selected_ref.shape[1]):
        picked_ref[pl.ds((k + 1) * rows, rows), :] = slices_ref[selected_ref[0, k]]


def attend_kernel(q_ref, g_ref, k_ref, half_ref, ds_ref, share_ref):
    heads, key_width, tokens = q_ref.shape
    value_width = g_ref.shape[2]
    scale = key_width ** (-0.5)
    cores, chips, rows, _ = share_ref.shape
    q = jnp.concatenate([q_ref[h] for h in range(heads)], axis=1)
    g = g_ref[...].reshape(tokens * heads, value_width)
    g = dot(order_matrix(tokens, heads), g).astype(BF16)
    keys = k_ref[...]
    values = keys[:, :value_width]
    step = 2 * tokens
    for at in range(0, heads * tokens, step):
        scores = dot(keys, q[:, at : at + step]) * scale
        top = jnp.max(scores, axis=0, keepdims=True)
        exps = jnp.exp(scores - top)
        probs = exps * (1.0 / jnp.sum(exps, axis=0, keepdims=True))
        half = probs.astype(BF16)
        half_ref[:, at : at + step] = half
        grad_prob = dot(values, g[at : at + step], ((1,), (1,)))
        delta = jnp.sum(half.astype(F32) * grad_prob, axis=0, keepdims=True)
        ds_ref[:, at : at + step] = (probs * (grad_prob - delta) * scale).astype(BF16)
    key_grad = dot(ds_ref[...], q, ((1,), (1,)))
    value_grad = dot(half_ref[...], g)
    for chip in range(chips):
        for core in range(cores):
            lo = (chip * cores + core) * rows
            both = key_grad[lo : lo + rows, :value_width] + value_grad[lo : lo + rows]
            share_ref[core, chip, :, :value_width] = both.astype(BF16)
            share_ref[core, chip, :, value_width:] = key_grad[lo : lo + rows, value_width:].astype(BF16)


def finish_kernel(k_ref, half_ref, ds_ref, o_ref, dq_ref):
    heads, key_width, tokens = dq_ref.shape
    value_width = o_ref.shape[2]
    keys = k_ref[...]
    out = dot(half_ref[...], keys[:, :value_width], ((0,), (0,))).astype(BF16)
    out = dot(order_matrix(tokens, heads, True), out).astype(BF16)
    o_ref[...] = out.reshape(tokens, heads, value_width)
    grad = dot(keys, ds_ref[...], ((0,), (0,))).astype(BF16)
    for h in range(heads):
        dq_ref[h] = grad[:, h * tokens : (h + 1) * tokens]


def bundle_kernel(selected_ref, parts_ref, out_ref, own_ref, *, holders):
    chips, total, width = parts_ref.shape
    rows = own_ref.shape[0]
    share = jnp.sum(parts_ref[...].astype(F32), axis=0)
    own_ref[...] = share[:rows]
    sent = share[rows:].astype(BF16)
    for x in range(out_ref.shape[0]):
        out_ref[x, :, :width] = sent
        for k in range(total // rows - 1):
            spot = selected_ref[0, k] - x * holders
            code = jnp.where((spot >= 0) & (spot < holders), spot, -1).astype(F32)
            fill = jnp.full((rows, out_ref.shape[2] - width), code, F32).astype(BF16)
            out_ref[x, pl.ds(k * rows, rows), width:] = fill


def spread_kernel(parts_ref, out_ref):
    holders, rows, width = out_ref.shape
    parts = parts_ref[...].reshape(-1, parts_ref.shape[2])
    count = parts.shape[0]
    spot = parts[:, width : width + 1].astype(F32)
    at = lax.broadcasted_iota(jnp.int32, (count, holders * rows), 1)
    row = lax.broadcasted_iota(jnp.int32, (count, holders * rows), 0)
    hit = (spot == (at // rows).astype(F32)) & (row % rows == at % rows)
    dense = dot(hit.astype(F32).astype(BF16), parts[:, :width], ((0,), (0,))).astype(BF16)
    out_ref[...] = dense.reshape(holders, rows, width)


def total_kernel(parts_ref, own_ref, out_ref):
    out_ref[...] = jnp.sum(parts_ref[...].astype(F32), axis=0) + own_ref[...]


def call(kernel, ins, shapes, name, flops=0):
    several = isinstance(shapes, (list, tuple))
    cost = pl.CostEstimate(flops=flops, transcendentals=0, bytes_accessed=0) if flops else None
    return pl.pallas_call(
        kernel,
        out_shape=shapes,
        in_specs=ins,
        out_specs=[VMEM] * len(shapes) if several else VMEM,
        cost_estimate=cost,
        compiler_params=pltpu.CompilerParams(vmem_limit_bytes=12 << 20),
        name=name,
    )


def shards(queries, latents, grad_out, selected):
    row_share, key_width = latents.shape[1:]
    tokens, heads, _ = queries.shape
    value_width = grad_out.shape[2]
    key_blocks = selected.shape[1] + 1
    chips, cores = (lax.axis_size(a) for a in HEADS)
    nx, nz = (lax.axis_size(a) for a in SEQ)
    rows = key_blocks * row_share
    key_rows = rows * chips * cores
    shape = jax.ShapeDtypeStruct

    slices = lax.all_gather(latents, "sz", axis=0, tiled=True)
    slices = lax.all_gather(slices, "sx", axis=0, tiled=True)
    own = lax.axis_index(SEQ).astype(jnp.int32).reshape(1)
    picked = call(pick_kernel, [SMEM, SMEM, VMEM], shape((rows, key_width), BF16), "pick")(own, selected, slices)
    keys = lax.all_gather(picked, HEADS, axis=0, tiled=True)

    wide = heads * tokens
    half, grad_score, bundles = call(
        attend_kernel,
        [VMEM] * 3,
        [
            shape((key_rows, wide), BF16),
            shape((key_rows, wide), BF16),
            shape((cores, chips, rows, key_width), BF16),
        ],
        "attend",
        flops=4 * 2 * key_rows * wide * key_width,
    )(queries.transpose(1, 2, 0), grad_out, keys)

    bundles = jnp.sum(swap(bundles, "hc").astype(F32), axis=0).astype(BF16)
    sent, own_grad = call(
        functools.partial(bundle_kernel, holders=nz),
        [SMEM, VMEM],
        [shape((nx, rows - row_share, 640), BF16), shape((row_share, key_width), F32)],
        "bundle",
    )(selected, swap(bundles, "hy"))
    dense = call(spread_kernel, [VMEM], shape((nz, row_share, key_width), BF16), "spread")(swap(sent, "sx"))
    output, grad_query = call(
        finish_kernel,
        [VMEM] * 3,
        [shape((tokens, heads, value_width), BF16), shape((heads, key_width, tokens), BF16)],
        "finish",
        flops=3 * 2 * key_rows * wide * key_width,
    )(keys, half, grad_score)
    arrived = swap(dense, "sz")
    latent_grad = call(total_kernel, [VMEM, VMEM], shape((row_share, key_width), F32), "total")(arrived, own_grad)
    return output, grad_query.transpose(2, 0, 1), latent_grad[None]


def solution(mesh):
    split = Mesh(mesh.devices.reshape(mesh.shape["heads"] // 2, 2, 4, 16), ("hy", "hc", "sx", "sz"))
    placed = P(SEQ, HEADS, None)
    return jax.shard_map(
        shards,
        mesh=split,
        in_specs=(placed, placed, placed, P(SEQ, None)),
        out_specs=(placed, placed, placed),
        check_vma=False,
    )
```

```python
import functools

import jax
import jax.numpy as jnp
from jax import lax
from jax.experimental import pallas as pl
from jax.experimental.pallas import tpu as pltpu
from jax.sharding import Mesh
from jax.sharding import PartitionSpec as P

SEQ = ("sx", "sz")
HEADS = ("hy", "hc")
F32 = jnp.float32
BF16 = jnp.bfloat16
VMEM = pl.BlockSpec(memory_space=pltpu.VMEM)
SMEM = pl.BlockSpec(memory_space=pltpu.SMEM)


def swap(tiles, axis):
    return lax.all_to_all(tiles, axis, 0, 0, tiled=True)


def dot(a, b, dims=((1,), (0,))):
    return lax.dot_general(a, b, (dims, ((), ())), preferred_element_type=F32)


def order_matrix(tokens, heads, transposed=False):
    size = tokens * heads
    rows = lax.broadcasted_iota(jnp.int32, (size, size), 1 if transposed else 0)
    cols = lax.broadcasted_iota(jnp.int32, (size, size), 0 if transposed else 1)
    return ((rows % tokens) * heads + rows // tokens == cols).astype(BF16)


def copies_kernel(own_ref, core_ref, selected_ref, latents_ref, out_ref, ids_ref):
    count = selected_ref.shape[1]
    ids_ref[0] = own_ref[0]
    for k in range(count):
        ids_ref[k + 1] = selected_ref[0, k]
    ids_ref[count + 1] = core_ref[0]
    for z in range(out_ref.shape[0]):
        out_ref[z] = latents_ref[0]


def pick_kernel(ids_ref, slices_ref, picked_ref):
    rows = slices_ref.shape[1]
    for k in range(picked_ref.shape[0] // rows):
        picked_ref[pl.ds(k * rows, rows), :] = slices_ref[ids_ref[k]]


def core_rows(ref, core, chips, cores, rows):
    starts = [pl.multiple_of((chip * cores + core) * rows, 8) for chip in range(chips)]
    return jnp.concatenate([ref[pl.ds(start, rows), :] for start in starts], axis=0)


def shares_of(core, half_ref, ds_ref, q, g, out_ref):
    chips, rows, _ = out_ref.shape
    cores = ds_ref.shape[0] // (chips * rows)
    value_width = g.shape[1]
    key_grad = dot(core_rows(ds_ref, core, chips, cores, rows), q, ((1,), (1,)))
    value_grad = dot(core_rows(half_ref, core, chips, cores, rows), g)
    for chip in range(chips):
        lo = chip * rows
        both = key_grad[lo : lo + rows, :value_width] + value_grad[lo : lo + rows]
        out_ref[chip, :, :value_width] = both.astype(out_ref.dtype)
        out_ref[chip, :, value_width:] = key_grad[lo : lo + rows, value_width:].astype(out_ref.dtype)


def attend_kernel(ids_ref, q_ref, g_ref, k_ref, half_ref, ds_ref, wide_q_ref, wide_g_ref, share_ref):
    heads, key_width, tokens = q_ref.shape
    value_width = g_ref.shape[2]
    scale = key_width ** (-0.5)
    q = jnp.concatenate([q_ref[h] for h in range(heads)], axis=1)
    wide_q_ref[...] = q
    g = g_ref[...].reshape(tokens * heads, value_width)
    g = dot(order_matrix(tokens, heads), g).astype(BF16)
    wide_g_ref[...] = g
    keys = k_ref[...]
    values = keys[:, :value_width]
    step = 2 * tokens
    for at in range(0, heads * tokens, step):
        scores = dot(keys, q[:, at : at + step]) * scale
        top = jnp.max(scores, axis=0, keepdims=True)
        exps = jnp.exp(scores - top)
        probs = exps * (1.0 / jnp.sum(exps, axis=0, keepdims=True))
        half = probs.astype(BF16)
        half_ref[:, at : at + step] = half
        grad_prob = dot(values, g[at : at + step], ((1,), (1,)))
        delta = jnp.sum(half.astype(F32) * grad_prob, axis=0, keepdims=True)
        ds_ref[:, at : at + step] = (probs * (grad_prob - delta) * scale).astype(BF16)
    shares_of(1 - ids_ref[ids_ref.shape[0] - 1], half_ref, ds_ref, q, g, share_ref)


def own_kernel(ids_ref, half_ref, ds_ref, wide_q_ref, wide_g_ref, share_ref):
    shares_of(ids_ref[ids_ref.shape[0] - 1], half_ref, ds_ref, wide_q_ref[...], wide_g_ref[...], share_ref)


def finish_kernel(k_ref, half_ref, ds_ref, o_ref, dq_ref):
    heads, key_width, tokens = dq_ref.shape
    value_width = o_ref.shape[2]
    keys = k_ref[...]
    out = dot(half_ref[...], keys[:, :value_width], ((0,), (0,))).astype(BF16)
    out = dot(order_matrix(tokens, heads, True), out).astype(BF16)
    o_ref[...] = out.reshape(tokens, heads, value_width)
    grad = dot(keys, ds_ref[...], ((0,), (0,))).astype(BF16)
    for h in range(heads):
        dq_ref[h] = grad[:, h * tokens : (h + 1) * tokens]


def bundle_kernel(ids_ref, parts_ref, out_ref, own_ref, *, holders):
    chips, total, width = parts_ref.shape
    rows = own_ref.shape[0]
    share = jnp.sum(parts_ref[...].astype(F32), axis=0)
    own_ref[...] = share[:rows]
    sent = share[rows:].astype(BF16)
    for x in range(out_ref.shape[0]):
        out_ref[x, :, :width] = sent
        for k in range(total // rows - 1):
            spot = ids_ref[k + 1] - x * holders
            code = jnp.where((spot >= 0) & (spot < holders), spot, -1).astype(F32)
            fill = jnp.full((rows, out_ref.shape[2] - width), code, F32).astype(BF16)
            out_ref[x, pl.ds(k * rows, rows), width:] = fill


def spread_kernel(parts_ref, out_ref):
    holders, rows, width = out_ref.shape
    parts = parts_ref[...].reshape(-1, parts_ref.shape[2])
    count = parts.shape[0]
    spot = parts[:, width : width + 1].astype(F32)
    at = lax.broadcasted_iota(jnp.int32, (count, holders * rows), 1)
    row = lax.broadcasted_iota(jnp.int32, (count, holders * rows), 0)
    hit = (spot == (at // rows).astype(F32)) & (row % rows == at % rows)
    dense = dot(hit.astype(F32).astype(BF16), parts[:, :width], ((0,), (0,))).astype(BF16)
    out_ref[...] = dense.reshape(holders, rows, width)


def total_kernel(parts_ref, own_ref, out_ref):
    out_ref[...] = jnp.sum(parts_ref[...].astype(F32), axis=0) + own_ref[...]


def call(kernel, ins, shapes, name, flops=0, out_specs=None):
    several = isinstance(shapes, (list, tuple))
    cost = pl.CostEstimate(flops=flops, transcendentals=0, bytes_accessed=0) if flops else None
    return pl.pallas_call(
        kernel,
        out_shape=shapes,
        in_specs=ins,
        out_specs=out_specs or ([VMEM] * len(shapes) if several else VMEM),
        cost_estimate=cost,
        compiler_params=pltpu.CompilerParams(vmem_limit_bytes=12 << 20),
        name=name,
    )


def shards(queries, latents, grad_out, selected):
    row_share, key_width = latents.shape[1:]
    tokens, heads, _ = queries.shape
    value_width = grad_out.shape[2]
    key_blocks = selected.shape[1] + 1
    chips, cores = (lax.axis_size(a) for a in HEADS)
    nx, nz = (lax.axis_size(a) for a in SEQ)
    rows = key_blocks * row_share
    key_rows = rows * chips * cores
    shape = jax.ShapeDtypeStruct

    own = lax.axis_index(SEQ).astype(jnp.int32).reshape(1)
    core = lax.axis_index("hc").astype(jnp.int32).reshape(1)
    copies, ids = call(
        copies_kernel,
        [SMEM] * 3 + [VMEM],
        [shape((nz, row_share, key_width), BF16), shape((key_blocks + 1,), jnp.int32)],
        "copies",
        out_specs=[VMEM, SMEM],
    )(own, core, selected, latents)
    slices = swap(copies, "sz")
    slices = swap(jnp.broadcast_to(slices[None], (nx, *slices.shape)), "sx")
    slices = slices.reshape(nx * nz, row_share, key_width)
    picked = call(pick_kernel, [SMEM, VMEM], shape((rows, key_width), BF16), "pick")(ids, slices)
    keys = lax.all_gather(picked, HEADS, axis=0, tiled=True)

    wide = heads * tokens
    half, grad_score, wide_q, wide_g, other_share = call(
        attend_kernel,
        [SMEM] + [VMEM] * 3,
        [
            shape((key_rows, wide), BF16),
            shape((key_rows, wide), BF16),
            shape((key_width, wide), BF16),
            shape((wide, value_width), BF16),
            shape((chips, rows, key_width), BF16),
        ],
        "attend",
        flops=3 * 2 * key_rows * wide * key_width,
    )(ids, queries.transpose(1, 2, 0), grad_out, keys)
    came = lax.ppermute(other_share, "hc", [(0, 1), (1, 0)])
    own_share = call(
        own_kernel,
        [SMEM] + [VMEM] * 4,
        shape((chips, rows, key_width), F32),
        "own",
        flops=2 * key_rows * wide * key_width,
    )(ids, half, grad_score, wide_q, wide_g)
    bundles = (own_share + came.astype(F32)).astype(BF16)
    sent, own_grad = call(
        functools.partial(bundle_kernel, holders=nz),
        [SMEM, VMEM],
        [shape((nx, rows - row_share, 640), BF16), shape((row_share, key_width), F32)],
        "bundle",
    )(ids, swap(bundles, "hy"))
    dense = call(spread_kernel, [VMEM], shape((nz, row_share, key_width), BF16), "spread")(swap(sent, "sx"))
    output, grad_query = call(
        finish_kernel,
        [VMEM] * 3,
        [shape((tokens, heads, value_width), BF16), shape((heads, key_width, tokens), BF16)],
        "finish",
        flops=3 * 2 * key_rows * wide * key_width,
    )(keys, half, grad_score)
    arrived = swap(dense, "sz")
    latent_grad = call(total_kernel, [VMEM, VMEM], shape((row_share, key_width), F32), "total")(arrived, own_grad)
    return output, grad_query.transpose(2, 0, 1), latent_grad[None]


def solution(mesh):
    split = Mesh(mesh.devices.reshape(mesh.shape["heads"] // 2, 2, 4, 16), ("hy", "hc", "sx", "sz"))
    placed = P(SEQ, HEADS, None)
    return jax.shard_map(
        shards,
        mesh=split,
        in_specs=(placed, placed, placed, P(SEQ, None)),
        out_specs=(placed, placed, placed),
        check_vma=False,
    )
```
